256 devices in a mesh: trial: 2 (over core), qa: 16 (over y, x), qb: 8 (over z).
Axes of the slice: x: 4, y: 4, z: 8, core: 2. Of those that a mesh axis runs over, the one named last changes fastest.
Arguments:
- wave_parts: float32 [4, 512, 128, 128], P('trial', ('qa', 'qb')), parts along dimension 0, may hold values from -6 to 6
- level_table: float32 [1024, 128, 128], P(('trial', 'qa', 'qb')), parts along dimension 0, may hold values from -2 to 2
- diagonal_angles: float32 [6, 128], P('trial'), parts along dimension 0, may hold values from 0.3 to 1.2
- turn_angles: float32 [6, 4], P('trial'), parts along dimension 0, may hold values from 0.3 to 1.2
Outputs:
- final_parts: float32 [4, 512, 128, 128], P('trial', ('qa', 'qb')), parts along dimension 0
The draws below stay inside these ranges and needn't reach their ends.
There are 2 independent parts, one for each index of `trial`. The reference program is written for one: setup_inputs(seed, part) draws one part's arguments, and reference() takes and returns one part's arrays. A program takes and returns all parts, laid end to end along the dimension named above; each array names one. Nothing has to cross between parts.
All inputs are finite; a program needn't handle non-finite values.
Results may differ from the reference program's by a relative error of at most 0.0003.
Values sent between devices are 32-bit elements.
A program may use at most 64 MiB of HBM per device.

```python
import jax
import jax.numpy as jnp
from jax import lax

BLOCKS_DEV = 4
ROWS = 128
LANES = 128
BLOCKS = 512
LAYERS = 3
N_QA = 16
N_QB = 8


def block_scale(own_key, dims, pieces, smallest, high):
    def one(position, blocks):
        heights = jax.random.uniform(jax.random.fold_in(jax.random.fold_in(own_key, 6), position), (blocks,), jnp.float32, smallest / len(pieces), high / len(pieces))
        return jnp.repeat(jnp.exp(heights), dims[position] // blocks).reshape((-1,) + (1,) * (len(dims) - position - 1))

    factor_of = one(*pieces[0])
    for cut in pieces[1:]:
        factor_of = factor_of * one(*cut)
    return factor_of


def scatter_about(rng, dims, spread, most, cuts=(), kind=jnp.bfloat16):
    values = spread * jax.random.normal(rng, dims, jnp.float32)
    if cuts:
        values = values * block_scale(rng, dims, cuts, -0.22, 0.18)
    return jnp.clip(values, -most, most).astype(kind)


def setup_inputs(seed: int = 0, part: int = 0) -> dict:
    key_of = jax.random.split(jax.random.key(seed), 5)
    own_keys = jax.random.split(jax.random.fold_in(key_of[4], part), 5)
    wave_parts = scatter_about(own_keys[0], (2, BLOCKS, ROWS, LANES), 1.0, 6.0, ((1, 128),), jnp.float32)
    level_table = jnp.clip(jax.random.uniform(own_keys[1], (BLOCKS, ROWS, LANES), jnp.float32, -2.0, 2.0) * block_scale(own_keys[1], (BLOCKS, ROWS, LANES), ((0, 128),), -0.4, 0.0), -2.0, 2.0)
    diagonal_angles = jnp.clip(jax.random.uniform(own_keys[2], (LAYERS, LANES), jnp.float32, 0.3, 1.2), 0.3, 1.2)
    turn_angles = jnp.clip(jax.random.uniform(own_keys[3], (LAYERS, 4), jnp.float32, 0.3, 1.2), 0.3, 1.2)
    return dict(wave_parts=wave_parts, level_table=level_table, diagonal_angles=diagonal_angles, turn_angles=turn_angles)


def count_bits(values, count):
    places = jnp.arange(count.bit_length() - 1, dtype=jnp.int32)
    return jnp.sum((values[..., None] >> places) & 1, axis=-1)


def rotation_table(count, angle):
    rank = jnp.arange(count, dtype=jnp.int32)
    apart = count_bits(rank[:, None] ^ rank[None, :], count)
    bits = count.bit_length() - 1
    size = jnp.cos(angle) ** (bits - apart).astype(jnp.float32) * jnp.sin(angle) ** apart.astype(jnp.float32)
    real_sign = jnp.where(apart % 4 == 0, 1.0, jnp.where(apart % 4 == 2, -1.0, 0.0)).astype(jnp.float32)
    imag_sign = jnp.where(apart % 4 == 1, -1.0, jnp.where(apart % 4 == 3, 1.0, 0.0)).astype(jnp.float32)
    return size * real_sign, size * imag_sign


def mix_dim(values, dim, angle):
    real_part, imag_part = rotation_table(values.shape[dim], angle)
    def times(table):
        moved = jnp.tensordot(values, table, axes=([dim], [0]), precision=lax.Precision.HIGHEST)
        return jnp.moveaxis(moved, -1, dim)
    by_real = times(real_part)
    by_imag = times(imag_part)
    return jnp.stack([by_real[0] - by_imag[1], by_real[1] + by_imag[0]])


def phase_step(values, levels, angle):
    turn = angle * levels
    return jnp.stack([values[0] * jnp.cos(turn) + values[1] * jnp.sin(turn), values[1] * jnp.cos(turn) - values[0] * jnp.sin(turn)])


def reference(wave_parts, level_table, diagonal_angles, turn_angles):
    values = wave_parts
    for layer in range(LAYERS):
        values = phase_step(values, level_table, diagonal_angles[layer])
        values = mix_dim(values, 3, turn_angles[layer, 0])
        values = mix_dim(values, 2, turn_angles[layer, 1])
        parts = values.reshape(2, N_QA, N_QB, BLOCKS_DEV, ROWS, LANES)
        parts = mix_dim(parts, 1, turn_angles[layer, 2])
        parts = mix_dim(parts, 2, turn_angles[layer, 3])
        parts = mix_dim(parts, 3, turn_angles[layer, 2])
        values = parts.reshape(values.shape)
    return values
```

```python
import jax
import jax.numpy as jnp
from jax import lax
from jax.experimental import pallas as pl
from jax.experimental.pallas import tpu as pltpu
from jax.sharding import PartitionSpec as P

MESH = pl.DeviceIdType.MESH
N = 128
F32, BF16 = jnp.float32, jnp.bfloat16
NN = (((1,), (0,)), ((), ()))
NT = (((1,), (1,)), ((), ()))
LANE, ROW, QUBITS = (0,) * 7, (1,) * 7, (3, 3, 3, 2, 2, 2, 2)
TABLES = ((0, ROW), (0, LANE), (0, QUBITS), (1, QUBITS), (1, LANE), (1, ROW), (2, ROW), (2, QUBITS), (2, LANE))


def cos_sin(x):
    y = x * 0.5
    z = y * y
    s = z * (-1.0 / 39916800.0) + 1.0 / 362880.0
    for k in (-1.0 / 5040.0, 1.0 / 120.0, -1.0 / 6.0, 1.0):
        s = s * z + k
    c = z * (1.0 / 479001600.0) - 1.0 / 3628800.0
    for k in (1.0 / 40320.0, -1.0 / 720.0, 1.0 / 24.0, -0.5, 1.0):
        c = c * z + k
    s = s * y
    return 1.0 - 2.0 * s * s, 2.0 * s * c


def split(x):
    high = x.astype(BF16)
    return high, (x - high.astype(F32)).astype(BF16)


def dot3(a, b, dims):
    dot = lambda u, v: lax.dot_general(u, v, dims, preferred_element_type=F32)
    return dot(a[0], b[0]) + (dot(a[0], b[1]) + dot(a[1], b[0]))


def strided(part, step):
    return pl.ds(part, N, stride=step)


def kernel(
    wave_hbm, level_hbm, diag_ref, turn_ref, out_ref,
    wave, level, high, low, mixed, cos_ref, sin_ref,
    send_b, send_lb, send_lc, send_c, send_a, got_b, got_lb, got_lc, got_c, got_a,
    load_sem, send_sem, recv_sem,
):
    trial, qa, qb = lax.axis_index("trial"), lax.axis_index("qa"), lax.axis_index("qb")
    me = qa * 8 + qb

    def peer(k):
        p = lax.rem(me + k, N)
        return p, (trial, p // 8, lax.rem(p, 8))

    barrier = pltpu.get_barrier_semaphore()

    @pl.loop(1, N)
    def _(k):
        pl.semaphore_signal(barrier, inc=1, device_id=peer(k)[1], device_id_type=MESH)

    loads = [
        pltpu.make_async_copy(level_hbm, level, load_sem.at[0]),
        pltpu.make_async_copy(wave_hbm, wave, load_sem.at[1]),
    ]
    for load in loads:
        load.start()

    def exchange(slot, source, target, rows):
        @pl.loop(1, N)
        def _(k):
            p, where = peer(k)
            pltpu.make_async_remote_copy(
                source.at[pl.ds(pl.multiple_of(p * rows, rows), rows)],
                target.at[pl.ds(pl.multiple_of(me * rows, rows), rows)],
                send_sem.at[slot],
                recv_sem.at[slot],
                device_id=where,
                device_id_type=MESH,
            ).start()

        own = pl.ds(pl.multiple_of(me * rows, rows), rows)
        target[own, :] = source[own, :]

    def arrive(slot, target, rows):
        span = target.at[pl.ds(0, (N - 1) * rows)]
        pltpu.make_async_copy(span, span, recv_sem.at[slot]).wait()

    def sent(slot, source, rows):
        span = source.at[pl.ds(0, (N - 1) * rows)]
        pltpu.make_async_copy(span, span, send_sem.at[slot]).wait()

    row_i = lax.broadcasted_iota(jnp.int32, (N, N), 0)
    col_i = lax.broadcasted_iota(jnp.int32, (N, N), 1)

    def build(index):
        layer, groups = TABLES[index]
        pairs = {g: cos_sin(jnp.full((1, N), turn_ref[layer, g], F32)) for g in sorted(set(groups))}
        total = None
        for place, g in enumerate(groups):
            c, s = pairs[g]
            own, other = (row_i >> place) & 1, (col_i >> place) & 1
            term = jnp.where(own == other, c, jnp.where(own == 1, s, -s))
            total = term if total is None else total * term
        high[index], low[index] = split(total)

    def table(index):
        return high[index], low[index]

    def mix_blocks(layer, source):
        c, s = cos_sin(jnp.full((1, N), turn_ref[layer, 2], F32))

        @pl.loop(0, 2)
        def _(part):
            u = [source[strided(part * 4 + block, 8), :] for block in range(4)]
            for i, j in ((0, 1), (2, 3), (0, 2), (1, 3)):
                u[i], u[j] = c * u[i] - s * u[j], s * u[i] + c * u[j]
            for block in range(4):
                mixed[part * 4 + block] = u[block]

    build(0)
    build(1)
    loads[0].wait()
    for block in range(4):
        send_lb[strided(block, 4), :] = level[block]
        send_lc[strided(block, 4), :] = level[block].T
    loads[1].wait()

    ones = jnp.zeros((N, N), jnp.int32)
    for place in range(7):
        ones = ones + ((row_i >> place) & 1) + ((col_i >> place) & 1)
    mine = 0
    for place in range(7):
        mine = mine + lax.rem(me // (1 << place), 2)

    @pl.loop(0, 4)
    def _(block):
        c, s = cos_sin(diag_ref[0:1, :] * level[block])
        m = (ones + (mine + block // 2 + lax.rem(block, 2))) & 3
        odd, sign = (m & 1) == 1, jnp.where(m >= 2, -1.0, 1.0)
        real, imag = sign * jnp.where(odd, s, c), sign * jnp.where(odd, c, -s)
        u, v = wave[0, block], wave[1, block]
        both = jnp.concatenate([u * real - v * imag, u * imag + v * real], axis=1)
        both = dot3(table(0), split(both), NN)
        both = jnp.concatenate([both[:, :N], both[:, N:]], axis=0)
        both = dot3(split(both), table(1), NT)
        send_b[strided(block, 8), :] = both[:N]
        send_b[strided(block + 4, 8), :] = both[N:]

    pl.semaphore_wait(barrier, N - 1)
    exchange(0, send_lb, got_lb, 4)
    exchange(1, send_b, got_b, 8)
    exchange(2, send_lc, got_lc, 4)

    def stage(layer, got, slot, first, angle, sending, levels):
        arrive(slot, got, 8)
        mix_blocks(layer, got)

        @pl.loop(0, 4)
        def _(block):
            both = jnp.concatenate([mixed[block], mixed[block + 4]], axis=1)
            both = dot3(table(first), split(both), NN)
            c, s = cos_ref[block], sin_ref[block]
            u, v = both[:, :N], both[:, N:]
            both = jnp.concatenate([u * c + v * s, v * c - u * s], axis=1)
            both = dot3(table(first + 1), split(both), NN)
            sending[strided(block, 8), :] = dot3(table(first + 2), split(both[:, :N]), NT)
            sending[strided(block + 4, 8), :] = dot3(table(first + 2), split(both[:, N:]), NT)

    for index in range(2, 9):
        build(index)
    arrive(0, got_lb, 4)

    @pl.loop(0, 4)
    def _(block):
        cos_ref[block], sin_ref[block] = cos_sin(diag_ref[1:2, :] * got_lb[strided(block, 4), :])

    stage(0, got_b, 1, 2, None, send_c, None)
    exchange(3, send_c, got_c, 8)

    angle = jnp.sum(jnp.where(col_i[0:1] == me, diag_ref[2:3, :], 0.0), axis=1, keepdims=True)
    arrive(2, got_lc, 4)

    @pl.loop(0, 4)
    def _(block):
        cos_ref[block], sin_ref[block] = cos_sin(angle * got_lc[strided(block, 4), :].T)

    stage(1, got_c, 3, 5, None, send_a, None)
    exchange(4, send_a, got_a, 8)

    arrive(4, got_a, 8)
    mix_blocks(2, got_a)

    @pl.loop(0, 4)
    def _(block):
        both = jnp.concatenate([mixed[block], mixed[block + 4]], axis=1)
        both = dot3(table(8), split(both), NN)
        u, v = both[:, :N].T, both[:, N:].T
        m = (4 - ((ones + (mine + block // 2 + lax.rem(block, 2))) & 3)) & 3
        odd, sign = (m & 1) == 1, jnp.where(m >= 2, -1.0, 1.0)
        out_ref[0, block] = sign * jnp.where(odd, -v, u)
        out_ref[1, block] = sign * jnp.where(odd, u, v)

    for slot, source, rows in ((0, send_lb, 4), (1, send_b, 8), (2, send_lc, 4), (3, send_c, 8), (4, send_a, 8)):
        sent(slot, source, rows)


def shards(wave_parts, level_table, diagonal_angles, turn_angles):
    wide, half = pltpu.VMEM((N * 8, N), F32), pltpu.VMEM((N * 4, N), F32)
    return pl.pallas_call(
        kernel,
        out_shape=jax.ShapeDtypeStruct((2, 4, N, N), F32),
        in_specs=[
            pl.BlockSpec(memory_space=pl.ANY),
            pl.BlockSpec(memory_space=pl.ANY),
            pl.BlockSpec(memory_space=pltpu.VMEM),
            pl.BlockSpec(memory_space=pltpu.SMEM),
        ],
        out_specs=pl.BlockSpec(memory_space=pltpu.VMEM),
        scratch_shapes=[
            pltpu.VMEM((2, 4, N, N), F32),
            pltpu.VMEM((4, N, N), F32),
            pltpu.VMEM((9, N, N), BF16),
            pltpu.VMEM((9, N, N), BF16),
            pltpu.VMEM((8, N, N), F32),
            pltpu.VMEM((4, N, N), F32),
            pltpu.VMEM((4, N, N), F32),
            wide, half, half, wide, wide,
            wide, half, half, wide, wide,
            pltpu.SemaphoreType.DMA((2,)),
            pltpu.SemaphoreType.DMA((5,)),
            pltpu.SemaphoreType.DMA((5,)),
        ],
        compiler_params=pltpu.CompilerParams(collective_id=0, has_side_effects=True),
        name="layers",
    )(wave_parts, level_table, diagonal_angles, turn_angles)


def solution(mesh):
    wave = P("trial", ("qa", "qb"), None, None)
    return jax.shard_map(
        shards,
        mesh=mesh,
        in_specs=(wave, P(("trial", "qa", "qb"), None, None), P("trial", None), P("trial", None)),
        out_specs=wave,
        check_vma=False,
    )
```

```python
import jax
import jax.numpy as jnp
from jax import lax
from jax.experimental import pallas as pl
from jax.experimental.pallas import tpu as pltpu
from jax.sharding import PartitionSpec as P

MESH = pl.DeviceIdType.MESH
N = 128
F32, BF16 = jnp.float32, jnp.bfloat16
NN = (((1,), (0,)), ((), ()))
NT = (((1,), (1,)), ((), ()))
LANE, ROW, QUBITS = (0,) * 7, (1,) * 7, (3, 3, 3, 2, 2, 2, 2)
TABLES = ((0, ROW), (0, LANE), (0, QUBITS), (1, QUBITS), (1, LANE), (1, ROW), (2, ROW), (2, QUBITS), (2, LANE))


def cos_sin(x):
    y = x * 0.5
    z = y * y
    s = z * (-1.0 / 39916800.0) + 1.0 / 362880.0
    for k in (-1.0 / 5040.0, 1.0 / 120.0, -1.0 / 6.0, 1.0):
        s = s * z + k
    c = z * (1.0 / 479001600.0) - 1.0 / 3628800.0
    for k in (1.0 / 40320.0, -1.0 / 720.0, 1.0 / 24.0, -0.5, 1.0):
        c = c * z + k
    s = s * y
    return 1.0 - 2.0 * s * s, 2.0 * s * c


def split(x):
    high = x.astype(BF16)
    return high, (x - high.astype(F32)).astype(BF16)


def dot3(a, b, dims):
    dot = lambda u, v: lax.dot_general(u, v, dims, preferred_element_type=F32)
    return dot(a[0], b[0]) + (dot(a[0], b[1]) + dot(a[1], b[0]))


def strided(part, step):
    return pl.ds(part, N, stride=step)


def kernel(
    wave_hbm, level_hbm, diag_ref, turn_ref, out_ref,
    wave, level, high, low, mixed, cos_ref, sin_ref,
    send_b, send_lb, send_lc, send_c, send_a, got_b, got_lb, got_lc, got_c, got_a,
    load_sem, send_sem, recv_sem,
):
    trial, qa, qb = lax.axis_index("trial"), lax.axis_index("qa"), lax.axis_index("qb")
    me = qa * 8 + qb

    barrier = pltpu.get_barrier_semaphore()

    def others(visit):
        @pl.loop(0, 16)
        def _(u):
            y = lax.rem(qa // 4 + 2 + 3 * (u // 4), 4)
            x = lax.rem(qa + 2 + 3 * u, 4)
            for step in (4, 3, 5, 2, 6, 1, 7):
                visit((y * 4 + x) * 8 + lax.rem(qb + step, 8))

        @pl.loop(0, 5)
        def _(u):
            for k in (1, 2, 3):
                visit(lax.rem(qa + u * 3 + k, 16) * 8 + qb)

    @others
    def _(p):
        pl.semaphore_signal(barrier, inc=1, device_id=(trial, lax.div(p, 8), lax.rem(p, 8)), device_id_type=MESH)

    loads = [
        pltpu.make_async_copy(level_hbm, level, load_sem.at[0]),
        pltpu.make_async_copy(wave_hbm, wave, load_sem.at[1]),
    ]
    for load in loads:
        load.start()

    def exchange(slot, source, target, rows):
        own = pl.ds(pl.multiple_of(me * rows, rows), rows)

        @others
        def _(p):
            pltpu.make_async_remote_copy(
                source.at[pl.ds(pl.multiple_of(p * rows, rows), rows)],
                target.at[own],
                send_sem.at[slot],
                recv_sem.at[slot],
                device_id=(trial, lax.div(p, 8), lax.rem(p, 8)),
                device_id_type=MESH,
            ).start()

        target[own, :] = source[own, :]

    def arrive(slot, target, rows):
        span = target.at[pl.ds(0, (N - 1) * rows)]
        pltpu.make_async_copy(span, span, recv_sem.at[slot]).wait()

    def sent(slot, source, rows):
        span = source.at[pl.ds(0, (N - 1) * rows)]
        pltpu.make_async_copy(span, span, send_sem.at[slot]).wait()

    row_i = lax.broadcasted_iota(jnp.int32, (N, N), 0)
    col_i = lax.broadcasted_iota(jnp.int32, (N, N), 1)

    def build(index):
        layer, groups = TABLES[index]
        pairs = {g: cos_sin(jnp.full((1, N), turn_ref[layer, g], F32)) for g in sorted(set(groups))}
        total = None
        for place, g in enumerate(groups):
            c, s = pairs[g]
            own, other = (row_i >> place) & 1, (col_i >> place) & 1
            term = jnp.where(own == other, c, jnp.where(own == 1, s, -s))
            total = term if total is None else total * term
        high[index], low[index] = split(total)

    def table(index):
        return high[index], low[index]

    def mix_blocks(layer, source):
        c, s = cos_sin(jnp.full((1, N), turn_ref[layer, 2], F32))

        @pl.loop(0, 2, unroll=2)
        def _(part):
            u = [source[strided(part * 4 + block, 8), :] for block in range(4)]
            for i, j in ((0, 1), (2, 3), (0, 2), (1, 3)):
                u[i], u[j] = c * u[i] - s * u[j], s * u[i] + c * u[j]
            for block in range(4):
                mixed[part * 4 + block] = u[block]

    build(0)
    build(1)
    loads[0].wait()
    for block in range(4):
        send_lb[strided(block, 4), :] = level[block]
        send_lc[strided(block, 4), :] = level[block].T
    loads[1].wait()

    ones = jnp.zeros((N, N), jnp.int32)
    for place in range(7):
        ones = ones + ((row_i >> place) & 1) + ((col_i >> place) & 1)
    mine = 0
    for place in range(7):
        mine = mine + lax.rem(me // (1 << place), 2)

    @pl.loop(0, 4, unroll=4)
    def _(block):
        c, s = cos_sin(diag_ref[0:1, :] * level[block])
        m = (ones + (mine + block // 2 + lax.rem(block, 2))) & 3
        odd, sign = (m & 1) == 1, jnp.where(m >= 2, -1.0, 1.0)
        real, imag = sign * jnp.where(odd, s, c), sign * jnp.where(odd, c, -s)
        u, v = wave[0, block], wave[1, block]
        both = jnp.concatenate([u * real - v * imag, u * imag + v * real], axis=1)
        both = dot3(table(0), split(both), NN)
        both = jnp.concatenate([both[:, :N], both[:, N:]], axis=0)
        both = dot3(split(both), table(1), NT)
        send_b[strided(block, 8), :] = both[:N]
        send_b[strided(block + 4, 8), :] = both[N:]

    pl.semaphore_wait(barrier, N - 1)
    exchange(0, send_lb, got_lb, 4)
    exchange(1, send_b, got_b, 8)
    exchange(2, send_lc, got_lc, 4)

    def stage(layer, got, slot, first, sending):
        arrive(slot, got, 8)
        mix_blocks(layer, got)

        @pl.loop(0, 4, unroll=4)
        def _(block):
            both = jnp.concatenate([mixed[block], mixed[block + 4]], axis=1)
            both = dot3(table(first), split(both), NN)
            c, s = cos_ref[block], sin_ref[block]
            u, v = both[:, :N], both[:, N:]
            both = jnp.concatenate([u * c + v * s, v * c - u * s], axis=1)
            both = dot3(table(first + 1), split(both), NN)
            sending[strided(block, 8), :] = dot3(table(first + 2), split(both[:, :N]), NT)
            sending[strided(block + 4, 8), :] = dot3(table(first + 2), split(both[:, N:]), NT)

    for index in range(2, 9):
        build(index)
    arrive(0, got_lb, 4)

    @pl.loop(0, 4, unroll=4)
    def _(block):
        cos_ref[block], sin_ref[block] = cos_sin(diag_ref[1:2, :] * got_lb[strided(block, 4), :])

    stage(0, got_b, 1, 2, send_c)
    exchange(3, send_c, got_c, 8)

    angle = jnp.sum(jnp.where(col_i[0:1] == me, diag_ref[2:3, :], 0.0), axis=1, keepdims=True)
    arrive(2, got_lc, 4)

    @pl.loop(0, 4, unroll=4)
    def _(block):
        cos_ref[block], sin_ref[block] = cos_sin(angle * got_lc[strided(block, 4), :].T)

    stage(1, got_c, 3, 5, send_a)
    exchange(4, send_a, got_a, 8)

    arrive(4, got_a, 8)
    mix_blocks(2, got_a)

    @pl.loop(0, 4, unroll=4)
    def _(block):
        both = jnp.concatenate([mixed[block], mixed[block + 4]], axis=1)
        both = dot3(table(8), split(both), NN)
        u, v = both[:, :N].T, both[:, N:].T
        m = (4 - ((ones + (mine + block // 2 + lax.rem(block, 2))) & 3)) & 3
        odd, sign = (m & 1) == 1, jnp.where(m >= 2, -1.0, 1.0)
        out_ref[0, block] = sign * jnp.where(odd, -v, u)
        out_ref[1, block] = sign * jnp.where(odd, u, v)

    for slot, source, rows in ((0, send_lb, 4), (1, send_b, 8), (2, send_lc, 4), (3, send_c, 8), (4, send_a, 8)):
        sent(slot, source, rows)


def shards(wave_parts, level_table, diagonal_angles, turn_angles):
    wide, half = pltpu.VMEM((N * 8, N), F32), pltpu.VMEM((N * 4, N), F32)
    return pl.pallas_call(
        kernel,
        out_shape=jax.ShapeDtypeStruct((2, 4, N, N), F32),
        in_specs=[
            pl.BlockSpec(memory_space=pl.ANY),
            pl.BlockSpec(memory_space=pl.ANY),
            pl.BlockSpec(memory_space=pltpu.VMEM),
            pl.BlockSpec(memory_space=pltpu.SMEM),
        ],
        out_specs=pl.BlockSpec(memory_space=pltpu.VMEM),
        scratch_shapes=[
            pltpu.VMEM((2, 4, N, N), F32),
            pltpu.VMEM((4, N, N), F32),
            pltpu.VMEM((9, N, N), BF16),
            pltpu.VMEM((9, N, N), BF16),
            pltpu.VMEM((8, N, N), F32),
            pltpu.VMEM((4, N, N), F32),
            pltpu.VMEM((4, N, N), F32),
            wide, half, half, wide, wide,
            wide, half, half, wide, wide,
            pltpu.SemaphoreType.DMA((2,)),
            pltpu.SemaphoreType.DMA((5,)),
            pltpu.SemaphoreType.DMA((5,)),
        ],
        compiler_params=pltpu.CompilerParams(collective_id=0, has_side_effects=True),
        name="layers",
    )(wave_parts, level_table, diagonal_angles, turn_angles)


def solution(mesh):
    wave = P("trial", ("qa", "qb"), None, None)
    return jax.shard_map(
        shards,
        mesh=mesh,
        in_specs=(wave, P(("trial", "qa", "qb"), None, None), P("trial", None), P("trial", None)),
        out_specs=wave,
        check_vma=False,
    )
```

```python
import jax
import jax.numpy as jnp
from jax import lax
from jax.experimental import pallas as pl
from jax.experimental.pallas import tpu as pltpu
from jax.sharding import PartitionSpec as P

MESH = pl.DeviceIdType.MESH
N = 128
F32, BF16 = jnp.float32, jnp.bfloat16
NN = (((1,), (0,)), ((), ()))
NT = (((1,), (1,)), ((), ()))
LANE, ROW, QUBITS = (0,) * 7, (1,) * 7, (3, 3, 3, 2, 2, 2, 2)
TABLES = ((0, ROW), (0, LANE), (0, QUBITS), (1, QUBITS), (1, LANE), (1, ROW), (2, ROW), (2, QUBITS), (2, LANE))


def cos_sin(x):
    y = x * 0.5
    z = y * y
    s = z * (-1.0 / 39916800.0) + 1.0 / 362880.0
    for k in (-1.0 / 5040.0, 1.0 / 120.0, -1.0 / 6.0, 1.0):
        s = s * z + k
    c = z * (1.0 / 479001600.0) - 1.0 / 3628800.0
    for k in (1.0 / 40320.0, -1.0 / 720.0, 1.0 / 24.0, -0.5, 1.0):
        c = c * z + k
    s = s * y
    return 1.0 - 2.0 * s * s, 2.0 * s * c


def split(x):
    high = x.astype(BF16)
    return high, (x - high.astype(F32)).astype(BF16)


def dot3(a, b, dims):
    dot = lambda u, v: lax.dot_general(u, v, dims, preferred_element_type=F32)
    return dot(a[0], b[0]) + (dot(a[0], b[1]) + dot(a[1], b[0]))


def strided(part, step):
    return pl.ds(part, N, stride=step)


def kernel(
    wave_hbm, level_hbm, diag_ref, turn_ref, out_ref,
    wave, level, high, low, mixed, turned, cos_ref, sin_ref,
    send_b, got_b, send_lb, send_lc, got_lb, got_lc, send_c0, send_c1, got_c0, got_c1, send_a0, send_a1, got_a0, got_a1,
    load_sem, send_sem, recv_sem,
):
    send_c, got_c, send_a, got_a = (send_c0, send_c1), (got_c0, got_c1), (send_a0, send_a1), (got_a0, got_a1)
    trial, qa, qb = lax.axis_index("trial"), lax.axis_index("qa"), lax.axis_index("qb")
    me = qa * 8 + qb

    barrier = pltpu.get_barrier_semaphore()

    def others(visit):
        @pl.loop(0, 16)
        def _(u):
            y = lax.rem(qa // 4 + 2 + 3 * (u // 4), 4)
            x = lax.rem(qa + 2 + 3 * u, 4)
            for step in (4, 3, 5, 2, 6, 1, 7):
                visit((y * 4 + x) * 8 + lax.rem(qb + step, 8))

        @pl.loop(0, 5)
        def _(u):
            for k in (1, 2, 3):
                visit(lax.rem(qa + u * 3 + k, 16) * 8 + qb)

    @others
    def _(p):
        pl.semaphore_signal(barrier, inc=1, device_id=(trial, lax.div(p, 8), lax.rem(p, 8)), device_id_type=MESH)

    loads = [
        pltpu.make_async_copy(level_hbm, level, load_sem.at[0]),
        pltpu.make_async_copy(wave_hbm, wave, load_sem.at[1]),
    ]
    for load in loads:
        load.start()

    def exchange(slot, source, target, rows):
        own = pl.ds(pl.multiple_of(me * rows, rows), rows)

        @others
        def _(p):
            pltpu.make_async_remote_copy(
                source.at[pl.ds(pl.multiple_of(p * rows, rows), rows)],
                target.at[own],
                send_sem.at[slot],
                recv_sem.at[slot],
                device_id=(trial, lax.div(p, 8), lax.rem(p, 8)),
                device_id_type=MESH,
            ).start()

        target[own, :] = source[own, :]

    def arrive(slot, target, rows):
        span = target.at[pl.ds(0, (N - 1) * rows)]
        pltpu.make_async_copy(span, span, recv_sem.at[slot]).wait()

    def sent(slot, source, rows):
        span = source.at[pl.ds(0, (N - 1) * rows)]
        pltpu.make_async_copy(span, span, send_sem.at[slot]).wait()

    row_i = lax.broadcasted_iota(jnp.int32, (N, N), 0)
    col_i = lax.broadcasted_iota(jnp.int32, (N, N), 1)

    def build(index):
        layer, groups = TABLES[index]
        pairs = {g: cos_sin(jnp.full((1, N), turn_ref[layer, g], F32)) for g in sorted(set(groups))}
        total = None
        for place, g in enumerate(groups):
            c, s = pairs[g]
            own, other = (row_i >> place) & 1, (col_i >> place) & 1
            term = jnp.where(own == other, c, jnp.where(own == 1, s, -s))
            total = term if total is None else total * term
        high[index], low[index] = split(total)

    def table(index):
        return high[index], low[index]

    def mix_blocks(layer, source, target=None):
        c, s = cos_sin(jnp.full((1, N), turn_ref[layer, 2], F32))

        @pl.loop(0, 2)
        def _(part):
            u = [source(block, part) for block in range(4)]
            for i, j in ((0, 1), (2, 3), (0, 2), (1, 3)):
                u[i], u[j] = c * u[i] - s * u[j], s * u[i] + c * u[j]
            for block in range(4):
                if target is None:
                    mixed[block * 2 + part] = u[block]
                else:
                    target[block // 2][strided(block % 2 * 2 + part, 4), :] = u[block]

    build(0)
    build(1)
    loads[0].wait()
    for block in range(4):
        send_lb[strided(block, 4), :] = level[block]
        send_lc[strided(block, 4), :] = level[block].T
    loads[1].wait()

    ones = jnp.zeros((N, N), jnp.int32)
    for place in range(7):
        ones = ones + ((row_i >> place) & 1) + ((col_i >> place) & 1)
    mine = 0
    for place in range(7):
        mine = mine + lax.rem(me // (1 << place), 2)

    @pl.loop(0, 4)
    def _(block):
        c, s = cos_sin(diag_ref[0:1, :] * level[block])
        m = (ones + (mine + block // 2 + lax.rem(block, 2))) & 3
        odd, sign = (m & 1) == 1, jnp.where(m >= 2, -1.0, 1.0)
        real, imag = sign * jnp.where(odd, s, c), sign * jnp.where(odd, c, -s)
        u, v = wave[0, block], wave[1, block]
        both = jnp.concatenate([u * real - v * imag, u * imag + v * real], axis=1)
        both = dot3(table(0), split(both), NN)
        both = jnp.concatenate([both[:, :N], both[:, N:]], axis=0)
        both = dot3(split(both), table(1), NT)
        send_b[strided(block * 2, 8), :] = both[:N]
        send_b[strided(block * 2 + 1, 8), :] = both[N:]

    pl.semaphore_wait(barrier, N - 1)
    exchange(0, send_lb, got_lb, 4)
    exchange(1, send_b, got_b, 8)
    exchange(2, send_lc, got_lc, 4)

    def turn(block, first, sources, keep):
        both = jnp.concatenate(sources, axis=1)
        both = dot3(table(first), split(both), NN)
        c, s = cos_ref[block], sin_ref[block]
        u, v = both[:, :N], both[:, N:]
        both = jnp.concatenate([u * c + v * s, v * c - u * s], axis=1)
        both = dot3(table(first + 1), split(both), NN)
        for part in range(2):
            keep(part, dot3(table(first + 2), split(both[:, part * N : part * N + N]), NT))

    for index in range(2, 9):
        build(index)
    arrive(0, got_lb, 4)

    @pl.loop(0, 4)
    def _(block):
        cos_ref[block], sin_ref[block] = cos_sin(diag_ref[1:2, :] * got_lb[strided(block, 4), :])

    arrive(1, got_b, 8)
    mix_blocks(0, lambda block, part: got_b[strided(block * 2 + part, 8), :])

    @pl.loop(0, 4, unroll=4)
    def _(block):
        def keep(part, value):
            turned[block * 2 + part] = value

        turn(block, 2, [mixed[block * 2], mixed[block * 2 + 1]], keep)

    mix_blocks(1, lambda block, part: turned[block * 2 + part], send_c)
    exchange(3, send_c[0], got_c[0], 4)
    exchange(5, send_c[1], got_c[1], 4)

    angle = jnp.sum(jnp.where(col_i[0:1] == me, diag_ref[2:3, :], 0.0), axis=1, keepdims=True)
    arrive(2, got_lc, 4)

    @pl.loop(0, 4)
    def _(block):
        cos_ref[block], sin_ref[block] = cos_sin(angle * got_lc[strided(block, 4), :].T)

    for half, (came, goes) in enumerate(((3, 4), (5, 6))):
        arrive(came, got_c[half], 4)

        @pl.loop(0, 2)
        def _(block):
            def keep(part, value):
                send_a[half][strided(block * 2 + part, 4), :] = value

            turn(half * 2 + block, 5, [got_c[half][strided(block * 2 + part, 4), :] for part in range(2)], keep)

        exchange(goes, send_a[half], got_a[half], 4)

    arrive(4, got_a[0], 4)
    arrive(6, got_a[1], 4)
    mix_blocks(2, lambda block, part: got_a[block // 2][strided(block % 2 * 2 + part, 4), :])

    @pl.loop(0, 4, unroll=4)
    def _(block):
        both = jnp.concatenate([mixed[block * 2], mixed[block * 2 + 1]], axis=1)
        both = dot3(table(8), split(both), NN)
        u, v = both[:, :N].T, both[:, N:].T
        m = (4 - ((ones + (mine + block // 2 + lax.rem(block, 2))) & 3)) & 3
        odd, sign = (m & 1) == 1, jnp.where(m >= 2, -1.0, 1.0)
        out_ref[0, block] = sign * jnp.where(odd, -v, u)
        out_ref[1, block] = sign * jnp.where(odd, u, v)

    for slot, source, rows in (
        (0, send_lb, 4), (1, send_b, 8), (2, send_lc, 4), (3, send_c[0], 4), (5, send_c[1], 4), (4, send_a[0], 4), (6, send_a[1], 4)
    ):
        sent(slot, source, rows)


def shards(wave_parts, level_table, diagonal_angles, turn_angles):
    wide, half = pltpu.VMEM((N * 8, N), F32), pltpu.VMEM((N * 4, N), F32)
    return pl.pallas_call(
        kernel,
        out_shape=jax.ShapeDtypeStruct((2, 4, N, N), F32),
        in_specs=[
            pl.BlockSpec(memory_space=pl.ANY),
            pl.BlockSpec(memory_space=pl.ANY),
            pl.BlockSpec(memory_space=pltpu.VMEM),
            pl.BlockSpec(memory_space=pltpu.SMEM),
        ],
        out_specs=pl.BlockSpec(memory_space=pltpu.VMEM),
        scratch_shapes=[
            pltpu.VMEM((2, 4, N, N), F32),
            pltpu.VMEM((4, N, N), F32),
            pltpu.VMEM((9, N, N), BF16),
            pltpu.VMEM((9, N, N), BF16),
            pltpu.VMEM((8, N, N), F32),
            pltpu.VMEM((8, N, N), F32),
            pltpu.VMEM((4, N, N), F32),
            pltpu.VMEM((4, N, N), F32),
            wide, wide, *[half] * 12,
            pltpu.SemaphoreType.DMA((2,)),
            pltpu.SemaphoreType.DMA((7,)),
            pltpu.SemaphoreType.DMA((7,)),
        ],
        compiler_params=pltpu.CompilerParams(collective_id=0, has_side_effects=True),
        name="layers",
    )(wave_parts, level_table, diagonal_angles, turn_angles)


def solution(mesh):
    wave = P("trial", ("qa", "qb"), None, None)
    return jax.shard_map(
        shards,
        mesh=mesh,
        in_specs=(wave, P(("trial", "qa", "qb"), None, None), P("trial", None), P("trial", None)),
        out_specs=wave,
        check_vma=False,
    )
```
